32 devices in a mesh: gx: 4 (over z), gy: 8 (over y, x, core).
Axes of the slice: x: 2, y: 2, z: 4, core: 2. Of those that a mesh axis runs over, the one named last changes fastest.
Arguments:
- state_prev: float32 [128, 128, 512], P('gy', None, 'gx'), may hold values from -60 to 60
- diffusivity: float32 [128, 128, 512], P('gy', None, 'gx'), may hold values from 0.5 to 4
- vapour: float32 [128, 128, 512], P('gy', None, 'gx'), may hold values from 0.01 to 0.1
- cos_zenith: float32 [128, 512], P('gy', 'gx'), may hold values from 0.1 to 1
- albedo: float32 [128, 512], P('gy', 'gx'), may hold values from 0.05 to 0.8
- absorption: float32 [128, 112], replicated, may hold values from 0.005 to 1
- solar_weight: float32 [112], replicated, may hold values from 0.002 to 0.02
- day_mask: int32 [512], P(('gx', 'gy')), may hold values from 0 to 1, as said below
Outputs:
- state_next: float32 [128, 128, 512], P('gy', None, 'gx')
- residual: float32 [128, 128, 512], P('gy', None, 'gx')
- net_flux: float32 [128, 128, 512], P('gy', None, 'gx')
The draws below stay inside these ranges and needn't reach their ends.
Inputs may be any that keep to these rules, and one draw needn't show every extreme that they name: `day_mask`: exactly half of the 512 entries are 1, and some device holds only sunlit blocks.
All inputs are finite; a program needn't handle non-finite values.
Results may differ from the reference program's by a relative error of at most 0.00015.
Values sent between devices are 32-bit elements; how exact they have to be, the bound alone decides.
A program may use at most 128 MiB of HBM per device.

```python
import math
import jax
import jax.numpy as jnp
from jax import lax

CX = 128
LEV = 128
G = 112
ITERS = 5
NX = 512
NY = 128
NBLK = 512


def draw_state_prev(key, part):
    latitude = jnp.arange(NY, dtype=jnp.float32)[:, None, None]
    growth = 10.0 ** (latitude / max(NY - 1, 1))
    values = jax.random.normal(key, (NY, LEV, NX), jnp.float32) * growth
    return jnp.clip(values, -60.0, 60.0)


def draw_day_mask(key, part):
    tilt_key, noon_key = jax.random.split(jax.random.fold_in(key, 7))
    blocks_along = NBLK // NY
    tilt = jax.random.randint(tilt_key, (), 0, 2 * blocks_along + 1)
    noon = jax.random.randint(noon_key, (), 0, blocks_along)
    latitude = jnp.arange(NY, dtype=jnp.int32)
    slope = tilt * (2 * latitude + 1 - NY)
    half_width = blocks_along // 2
    offset_rows = jnp.sign(slope) * (jnp.abs(slope) // NY)
    day_width = half_width + jnp.clip(offset_rows, -half_width, half_width)
    longitude = jnp.arange(blocks_along, dtype=jnp.int32)
    distance = (longitude[:, None] - noon) % blocks_along
    sunlit = (distance < day_width[None, :]).astype(jnp.int32)
    return sunlit.reshape(NBLK)


def levels(own_key, extent, cuts, least, largest):
    gain, own = 1.0, jax.random.fold_in(own_key, 6)
    for position, parts in cuts:
        heights = jnp.exp(jax.random.uniform(jax.random.fold_in(own, position), (parts,), jnp.float32, least / len(cuts), largest / len(cuts)))
        gain = gain * jnp.repeat(heights, extent[position] // parts).reshape([-1 if axis == position else 1 for axis in range(len(extent))])
    return gain


def setup_inputs(seed: int = 0) -> dict:
    key_of = jax.random.split(jax.random.key(seed), 9)
    state_prev = draw_state_prev(jax.random.fold_in(key_of[8], 71), 0)
    diffusivity = jnp.clip(jnp.exp(math.log(4.0) - 2.0794415 * jax.random.uniform(key_of[1], (NY, LEV, NX), jnp.float32) ** levels(key_of[1], (NY, LEV, NX), ((0, 8), (2, 4)), -0.2, 0.2)), 0.5, 4.0)
    vapour = jnp.clip(jnp.exp(math.log(0.1) - 2.3025851 * jax.random.uniform(key_of[2], (NY, LEV, NX), jnp.float32) ** levels(key_of[2], (NY, LEV, NX), ((0, 8), (2, 4)), -0.2, 0.2)), 0.01, 0.1)
    cos_zenith = jnp.clip(0.1 + 0.9 * jax.random.uniform(key_of[3], (NY, NX), jnp.float32) ** levels(key_of[3], (NY, NX), ((0, 8), (1, 4)), -0.2, 0.2), 0.1, 1.0)
    albedo = jnp.clip(0.05 + 0.75 * jax.random.uniform(key_of[4], (NY, NX), jnp.float32) ** levels(key_of[4], (NY, NX), ((0, 8), (1, 4)), -0.2, 0.2), 0.05, 0.8)
    absorption = jnp.clip(jnp.exp(jax.random.uniform(key_of[5], (LEV, G), jnp.float32, math.log(0.005), math.log(1.0))), 0.005, 1.0)
    solar_weight = jnp.clip(jnp.exp(jax.random.uniform(key_of[6], (G,), jnp.float32, math.log(0.002), math.log(0.02))), 0.002, 0.02)
    day_mask = draw_day_mask(jax.random.fold_in(key_of[8], 71), 0)
    return dict(state_prev=state_prev, diffusivity=diffusivity, vapour=vapour, cos_zenith=cos_zenith, albedo=albedo, absorption=absorption, solar_weight=solar_weight, day_mask=day_mask)


def neighbours(values):
    widened = jnp.concatenate([values[:, :, -1:], values, values[:, :, :1]], 2)
    extended = jnp.pad(values, ((1, 1), (0, 0), (0, 0)))
    return (widened, extended)

def face_terms(diffusivity):
    widened, extended = neighbours(diffusivity)
    east_face = jnp.sqrt(diffusivity * widened[:, :, 2:])
    west_face = jnp.sqrt(diffusivity * widened[:, :, :-2])
    north_face = jnp.sqrt(diffusivity * extended[2:])
    south_face = jnp.sqrt(diffusivity * extended[:-2])
    level_face = jnp.sqrt(diffusivity[:, 1:] * diffusivity[:, :-1])
    return (east_face, west_face, north_face, south_face, level_face)

def operate(values, conductances):
    east_face, west_face, north_face, south_face, level_face = conductances
    widened, extended = neighbours(values)
    applied = values + east_face * (values - widened[:, :, 2:]) + west_face * (values - widened[:, :, :-2])
    applied = applied + north_face * (values - extended[2:]) + south_face * (values - extended[:-2])
    vertical = level_face * (values[:, 1:] - values[:, :-1])
    padding = jnp.zeros_like(values[:, :1])
    return applied - jnp.concatenate([vertical, padding], 1) + jnp.concatenate([padding, vertical], 1)

def reference(state_prev, diffusivity, vapour, cos_zenith, albedo, absorption, solar_weight, day_mask):
    conductances = face_terms(diffusivity)
    state_next = state_prev
    residual = state_prev - operate(state_prev, conductances)
    direction = residual
    current = jnp.sum(residual * residual)
    for iteration in range(ITERS):
        applied = operate(direction, conductances)
        step_size = current / jnp.sum(direction * applied)
        state_next = state_next + step_size * direction
        residual = residual - step_size * applied
        following = jnp.sum(residual * residual)
        direction = residual + following / current * direction
        current = following
    optical = vapour * (1.0 + 0.5 * jnp.tanh(state_prev))
    absorb32 = absorption.astype(jnp.float32)
    weight32 = solar_weight.astype(jnp.float32)

    def one_row(inputs):
        layer_amount, cosine, surface = inputs
        thickness = absorb32[:, :, None] * layer_amount[:, None, :]
        cumulative = jnp.cumsum(thickness, 0)
        downward = cosine * jnp.exp(-cumulative / cosine)
        upward = surface * downward[-1] * jnp.exp(-1.66 * (cumulative[-1] - cumulative))
        return jnp.einsum('lgc,g->lc', downward - upward, weight32, precision=lax.Precision.HIGHEST)
    fluxes = lax.map(one_row, (optical, cos_zenith, albedo))
    blocks_along = NBLK // NY
    lit_rows = jnp.repeat(day_mask.reshape(blocks_along, NY).T, CX, axis=1).astype(jnp.float32)
    net_flux = fluxes * lit_rows[:, None, :]
    return (state_next, residual, net_flux)
```

```python
import functools
import math

import jax
import jax.numpy as jnp
from jax import lax
from jax.experimental import pallas as pl
from jax.experimental.pallas import tpu as pltpu
from jax.sharding import PartitionSpec as P

ITERS = 5
SUB = 8
WINDOWS = ITERS + 3
UNROLL = 32
LOG2E = math.log2(math.e)
MESH = pl.DeviceIdType.MESH
F32 = jnp.float32


def edge(rows, w):
    return max(0, rows * (2 * w - 1) // (2 * WINDOWS))


def radiate(j, state, vapour_ref, cos_ref, albedo_ref, maskv_ref, wcol_ref, wide, scales, partial, net_ref):
    levels, gpoints, lanes = wide.shape
    down_scale, up_scale = scales.at[0], scales.at[1]
    cosine = cos_ref[pl.ds(j, 1), :]
    optical = vapour_ref[j] * (1.0 + 0.5 * jnp.tanh(state))
    down_scale[...] = optical * (-LOG2E / cosine)
    up_scale[...] = optical * (-1.66 * LOG2E)

    def downward(l, carry):
        carry = carry * jnp.exp2(wide[l] * down_scale[pl.ds(l, 1), :])
        partial[pl.ds(pl.multiple_of(l * SUB, SUB), SUB), :] = jnp.sum(
            carry.reshape(gpoints // SUB, SUB, lanes), 0
        )
        return carry

    carry = lax.fori_loop(0, levels, downward, wcol_ref[...] * cosine, unroll=UNROLL)
    carry = carry * albedo_ref[pl.ds(j, 1), :]

    def upward(i, carry):
        l = levels - 1 - i
        where = pl.ds(pl.multiple_of(l * SUB, SUB), SUB)
        partial[where, :] = partial[where, :] - jnp.sum(
            carry.reshape(gpoints // SUB, SUB, lanes), 0
        )
        return carry * jnp.exp2(wide[l] * up_scale[pl.ds(l, 1), :])

    lax.fori_loop(0, levels, upward, carry, unroll=UNROLL)
    total = partial[pl.ds(0, levels, stride=SUB), :]
    for s in range(1, SUB):
        total = total + partial[pl.ds(s, levels, stride=SUB), :]
    net_ref[j] = total * maskv_ref[pl.ds(j, 1), :]


def solve_kernel(
    nx, ny,
    state_hbm, diff_hbm, vapour_hbm, cos_hbm, albedo_hbm, mask_hbm, absorb_hbm, weight_hbm,
    basis, xs, ds, vapour_ref, cos_ref, albedo_ref, net_ref, wide, wcol, maskv, coef,
    root, degree, gain_d, inverse_d, absorb, weight_row, mask_smem,
    lon_send, lon_recv, lon_halo, scales, partial, sums, mine, stage_one, half_sum, stage_two,
    in_sem, lat_ssem, lat_rsem, lon_ssem, lon_rsem, one_ssem, one_rsem, two_ssem, two_rsem,
):
    rows, levels, lanes = vapour_ref.shape
    gpoints = wide.shape[1]
    tiles = levels // SUB
    per = lanes // (2 * tiles)
    groups = rows // per
    moments = 2 * ITERS + 1
    ix = lax.axis_index("gx")
    iy = lax.axis_index("gy")
    gx_east, gx_west = lax.rem(ix + 1, nx), lax.rem(ix + nx - 1, nx)
    inside = pl.ds(1, rows)

    loads = [
        pltpu.make_async_copy(src, dst, in_sem.at[i])
        for i, (src, dst) in enumerate([
            (diff_hbm, ds.at[inside]), (state_hbm, xs.at[inside]), (absorb_hbm, absorb),
            (weight_hbm, weight_row), (mask_hbm, mask_smem), (cos_hbm, cos_ref),
            (albedo_hbm, albedo_ref), (vapour_hbm, vapour_ref),
        ])
    ]
    for load in loads:
        load.start()

    barrier = pltpu.get_barrier_semaphore()
    for d in range(1, nx):
        pl.semaphore_signal(
            barrier, inc=1, device_id=(lax.rem(ix + d, nx), iy), device_id_type=MESH
        )
    for d in range(1, ny):
        pl.semaphore_signal(
            barrier, inc=1, device_id=(ix, lax.rem(iy + d, ny)), device_id_type=MESH
        )

    lane = lax.broadcasted_iota(jnp.int32, (SUB, lanes), 1)
    sub = lax.broadcasted_iota(jnp.int32, (SUB, lanes), 0)
    first_lane, last_lane = lane == 0, lane == lanes - 1
    first_sub, last_sub = sub == 0, sub == SUB - 1
    even_lane = (lane & 1) == 0
    zero = jnp.zeros((SUB, lanes), F32)

    def field(k):
        return ds if k == 0 else xs if k == 1 else basis.at[k - 2]

    def lat_copy(k, side):
        ref = field(k) if isinstance(k, int) else basis.at[k - 2]
        return pltpu.make_async_remote_copy(
            src_ref=ref.at[1 if side == 0 else rows],
            dst_ref=ref.at[rows + 1 if side == 0 else 0],
            send_sem=lat_ssem.at[k, side],
            recv_sem=lat_rsem.at[k, side],
            device_id=(ix, lax.rem(iy + ny - 1, ny) if side == 0 else lax.rem(iy + 1, ny)),
            device_id_type=MESH,
        )

    def lon_copy(k, side):
        return pltpu.make_async_remote_copy(
            src_ref=lon_send.at[k],
            dst_ref=lon_recv.at[k, side],
            send_sem=lon_ssem.at[k, side],
            recv_sem=lon_rsem.at[k, side],
            device_id=(gx_west if side == 0 else gx_east, iy),
            device_id_type=MESH,
        )

    def send_halo(k):
        @pl.when(iy > 0)
        def _():
            lat_copy(k, 0).start()

        @pl.when(iy < ny - 1)
        def _():
            lat_copy(k, 1).start()

        for side in range(2):
            lon_copy(k, side).start()

    def wait_halo(k):
        @pl.when(iy > 0)
        def _():
            lat_copy(k, 0).wait_send()
            lat_copy(k, 1).wait_recv()

        @pl.when(iy < ny - 1)
        def _():
            lat_copy(k, 1).wait_send()
            lat_copy(k, 0).wait_recv()

        for side in range(2):
            lon_copy(k, side).wait()

    def merged(k, g):
        west = lon_recv[k, 1, g * SUB:(g + 1) * SUB, :]
        east = pltpu.roll(lon_recv[k, 0, g * SUB:(g + 1) * SUB, :], lanes - 2, 1)
        return jnp.where(even_lane, west, east)

    bits = [((lane >> (1 + b)) & 1) == 1 for b in range((lanes // 2 - 1).bit_length())]

    def pack(pieces):
        level = [pltpu.roll(piece, (2 * q + 1) % lanes, 1) for q, piece in enumerate(pieces)]
        for mask in bits:
            level = [jnp.where(mask, b, a) for a, b in zip(level[::2], level[1::2])]
        return level[0]

    def group_rows(g):
        return pl.ds(pl.multiple_of(g * SUB, SUB), SUB)

    def lon_pair(value, halo, q):
        moved = pltpu.roll(halo, (lanes - 2 * q) % lanes, 1)
        return (
            jnp.where(last_lane, moved, pltpu.roll(value, lanes - 1, 1)),
            jnp.where(first_lane, moved, pltpu.roll(value, 1, 1)),
        )

    def vertical_pair(values):
        later = [pltpu.roll(v, 1, 0) for v in values]
        sooner = [pltpu.roll(v, SUB - 1, 0) for v in values]
        above = [jnp.where(first_sub, later[t - 1] if t else zero, later[t]) for t in range(tiles)]
        below = [
            jnp.where(last_sub, sooner[t + 1] if t < tiles - 1 else zero, sooner[t])
            for t in range(tiles)
        ]
        return above, below

    def plane_of(ref, j):
        return [ref[j, t * SUB:(t + 1) * SUB, :] for t in range(tiles)]

    def reduce_copy(r, stage, d):
        buffer = stage_one if stage == 0 else stage_two
        slot = ix if stage == 0 else iy
        ssem = one_ssem if stage == 0 else two_ssem
        rsem = one_rsem if stage == 0 else two_rsem
        peer = (lax.rem(ix + d, nx), iy) if stage == 0 else (ix, lax.rem(iy + d, ny))
        return pltpu.make_async_remote_copy(
            src_ref=(mine if stage == 0 else half_sum).at[r],
            dst_ref=buffer.at[r, slot],
            send_sem=ssem.at[r, d - 1],
            recv_sem=rsem.at[r, d - 1],
            device_id=peer,
            device_id_type=MESH,
        )

    def reduce_start(r, stage):
        source, buffer = (mine, stage_one) if stage == 0 else (half_sum, stage_two)
        n = nx if stage == 0 else ny
        buffer[r, ix if stage == 0 else iy] = source[r]
        for d in range(1, n):
            reduce_copy(r, stage, d).start()

    def reduce_end(r, stage):
        n = nx if stage == 0 else ny
        for d in range(1, n):
            reduce_copy(r, stage, d).wait()
        buffer = stage_one if stage == 0 else stage_two
        total = buffer[r, 0]
        for d in range(1, n):
            total = total + buffer[r, d]
        return total

    def all_lanes(values):
        shift = lanes // 2
        while shift:
            values = values + pltpu.roll(values, shift, 1)
            shift //= 2
        return values

    def window(first, last):
        @pl.loop(first, last)
        def _(j):
            radiate(
                j, xs[j + 1], vapour_ref, cos_ref, albedo_ref, maskv, wcol, wide, scales,
                partial, net_ref,
            )

    for k in range(2, 2 + ITERS):
        @pl.when(iy == 0)
        def _():
            basis[k - 2, 0] = jnp.zeros((levels, lanes), F32)

        @pl.when(iy == ny - 1)
        def _():
            basis[k - 2, rows + 1] = jnp.zeros((levels, lanes), F32)

    for k in range(2):
        loads[k].wait()
        if k == 0:
            pl.semaphore_wait(barrier, nx + ny - 2)

        @pl.loop(0, groups)
        def _(g):
            pieces = []
            for i in range(per):
                pieces += plane_of(field(k), g * per + i + 1)
            lon_send[k, group_rows(g), :] = pack(pieces)

        send_halo(k)

    def spread(j, total):
        part = zero
        for t in range(tiles):
            here = pl.ds(t * SUB, SUB)
            d = ds[j + 1, here, :]
            reciprocal = lax.rsqrt(d)
            root[j + 1, here, :] = d * reciprocal
            inverse_d[j, here, :] = reciprocal * reciprocal
            square = d * d
            part = part + square * square * square
        return total + part

    squares = lax.fori_loop(0, rows, spread, zero)
    mine[0] = jnp.concatenate([squares, jnp.zeros_like(squares)], 0)
    reduce_start(0, 0)

    for load in loads[2:]:
        load.wait()

    for j in range(rows):
        maskv[j:j + 1, :] = jnp.full((1, lanes), mask_smem[j].astype(F32), F32)
    column = jnp.broadcast_to(weight_row[...], (lanes, gpoints)).T
    wcol[...] = column

    spans = 4

    @pl.loop(0, spans)
    def _(i):
        span = levels // spans
        turned = pltpu.roll(absorb[...], lax.rem(levels - i * span, levels), 1)
        for m in range(span):
            wide[i * span + m] = jnp.broadcast_to(turned[:, m:m + 1], (gpoints, lanes))

    window(0, edge(rows, 1))
    half_sum[0] = reduce_end(0, 0)
    reduce_start(0, 1)

    wait_halo(0)
    wait_halo(1)

    @pl.when(iy > 0)
    def _():
        root[0] = ds[0] * lax.rsqrt(ds[0])

    @pl.when(iy == 0)
    def _():
        root[0] = jnp.zeros((levels, lanes), F32)
        xs[0] = jnp.zeros((levels, lanes), F32)

    @pl.when(iy < ny - 1)
    def _():
        root[rows + 1] = ds[rows + 1] * lax.rsqrt(ds[rows + 1])

    @pl.when(iy == ny - 1)
    def _():
        root[rows + 1] = jnp.zeros((levels, lanes), F32)
        xs[rows + 1] = jnp.zeros((levels, lanes), F32)

    for g in range(groups):
        d = merged(0, g)
        lon_halo[0, g * SUB:(g + 1) * SUB, :] = d * lax.rsqrt(d)
        lon_halo[1, g * SUB:(g + 1) * SUB, :] = merged(1, g)

    @pl.loop(0, groups)
    def _(g):
        root_halo = lon_halo[0, group_rows(g), :]
        x_halo = lon_halo[1, group_rows(g), :]
        pieces = []
        for i in range(per):
            j = g * per + i
            s_here, x_here = plane_of(root, j + 1), plane_of(xs, j + 1)
            s_above, s_below = vertical_pair(s_here)
            x_above, x_below = vertical_pair(x_here)
            for t in range(tiles):
                at = pl.ds(t * SUB, SUB)
                q = i * tiles + t
                s_pairs = lon_pair(s_here[t], root_halo, q) + (
                    root[j + 2, at, :], root[j, at, :], s_above[t], s_below[t]
                )
                x_pairs = lon_pair(x_here[t], x_halo, q) + (
                    xs[j + 2, at, :], xs[j, at, :], x_above[t], x_below[t]
                )
                around, change = None, None
                for s, x in zip(s_pairs, x_pairs):
                    term = s * (x - x_here[t])
                    around = s if around is None else around + s
                    change = term if change is None else change + term
                degree[j, at, :] = s_here[t] * around
                start = ds[j + 1, at, :] * change
                basis[0, j + 1, at, :] = start
                pieces.append(start)
        lon_send[2, group_rows(g), :] = pack(pieces)

    send_halo(2)
    window(edge(rows, 1), edge(rows, 2))
    squares = reduce_end(0, 1)
    count = nx * ny * rows * levels * lanes
    squares = all_lanes(jnp.sum(squares, 0, keepdims=True))
    half = 6.0 * jnp.exp(jnp.log(squares * (1.0 / count)) * (1.0 / 6.0))
    twice = jnp.broadcast_to(2.0 / half, (SUB, lanes))

    def advance(k, first, last):
        wait_halo(2 + k)
        for g in range(groups):
            lon_halo[0, g * SUB:(g + 1) * SUB, :] = merged(2 + k, g)
        here, there = basis.at[k], basis.at[k + 1]

        def step(g, totals):
            halo = lon_halo[0, group_rows(g), :]
            pieces = []
            parts = [zero] * len(totals)
            for i in range(per):
                j = g * per + i
                u = plane_of(here, j + 1)
                above, below = vertical_pair(u)
                for t in range(tiles):
                    at = pl.ds(t * SUB, SUB)
                    east, west = lon_pair(u[t], halo, i * tiles + t)
                    around = ((east + west) + (above[t] + below[t])) + (
                        here[j + 2, at, :] + here[j, at, :]
                    )
                    if first:
                        own = twice * degree[j, at, :] - 2.0
                        other = twice * ds[j + 1, at, :]
                        degree[j, at, :] = own
                        gain_d[j, at, :] = other
                        later = 0.5 * (own * u[t] - other * around)
                    else:
                        later = degree[j, at, :] * u[t] - gain_d[j, at, :] * around
                        later = later - basis[k - 1, j + 1, at, :]
                    there[j + 1, at, :] = later
                    weighed = later * inverse_d[j, at, :]
                    parts[0] = parts[0] + weighed * u[t]
                    parts[1] = parts[1] + weighed * later
                    if first:
                        parts[2] = parts[2] + (u[t] * inverse_d[j, at, :]) * u[t]
                    pieces.append(later)
            if not last:
                lon_send[3 + k, group_rows(g), :] = pack(pieces)
            return tuple(a + b for a, b in zip(totals, parts))

        totals = lax.fori_loop(0, groups, step, (zero,) * (3 if first else 2))
        sums[2 * k + 1] = totals[0]
        sums[2 * k + 2] = totals[1]
        if first:
            sums[0] = totals[2]

    for k in range(ITERS):
        advance(k, k == 0, k == ITERS - 1)
        if k < ITERS - 1:
            send_halo(3 + k)
            window(edge(rows, 2 + k), edge(rows, 3 + k))

    lines = [jnp.sum(sums[m], 0, keepdims=True) for m in range(moments)]
    lines += [jnp.zeros_like(lines[0])] * (2 * SUB - moments)
    mine[1] = jnp.concatenate(lines, 0)
    reduce_start(1, 0)
    window(edge(rows, ITERS + 1), edge(rows, ITERS + 2))
    half_sum[1] = reduce_end(1, 0)
    reduce_start(1, 1)
    window(edge(rows, ITERS + 2), edge(rows, ITERS + 3))
    values = all_lanes(reduce_end(1, 1))
    raw = [values[m:m + 1, :] for m in range(moments)]

    mu = [raw[0], raw[1]]
    for k in range(1, ITERS + 1):
        mu.append(2.0 * raw[2 * k] - mu[0])
        if k < ITERS:
            mu.append(2.0 * raw[2 * k + 1] - mu[1])
    gram = [
        [0.5 * (mu[i + j] + mu[abs(i - j)]) for j in range(ITERS + 1)] for i in range(ITERS + 1)
    ]

    def inner(a, b):
        terms = []
        for i in range(len(a)):
            for j in range(len(b)):
                terms.append((a[i] * b[j]) * gram[i][j])
        while len(terms) > 1:
            terms = [
                terms[i] + terms[i + 1] if i + 1 < len(terms) else terms[i]
                for i in range(0, len(terms), 2)
            ]
        return terms[0]

    centre = half + 1.0
    one = jnp.ones_like(half)
    none = jnp.zeros_like(half)
    res, direction, gain = [one], [one], [none] * ITERS
    current = inner(res, res)
    for iteration in range(ITERS):
        image = [centre * c for c in direction] + [none]
        for j, c in enumerate(direction):
            if j == 0:
                image[1] = image[1] + half * c
            else:
                image[j + 1] = image[j + 1] + 0.5 * half * c
                image[j - 1] = image[j - 1] + 0.5 * half * c
        step = current / inner(direction, image)
        for j, c in enumerate(direction):
            gain[j] = gain[j] + step * c
        res = [r - step * q for r, q in zip(res + [none], image)]
        if iteration < ITERS - 1:
            following = inner(res, res)
            ratio = following / current
            direction = [r + ratio * c for r, c in zip(res, direction + [none])]
            current = following

    lines = gain + res
    lines += [none] * (2 * SUB - len(lines))
    coef[...] = jnp.concatenate(lines, 0)


def finish_kernel(
    basis, xs, ds, vapour_ref, cos_ref, albedo_ref, net_ref, wide, wcol, maskv, coef,
    next_hbm, residual_hbm, net_hbm,
    next_ref, residual_ref, rest, scales, partial, sems,
):
    rows, levels, lanes = vapour_ref.shape
    tiles = levels // SUB
    done = edge(rows, WINDOWS)
    chunk = rows // 4
    early = pltpu.make_async_copy(
        net_ref.at[pl.ds(0, done)], net_hbm.at[pl.ds(0, done)], sems.at[0, 0]
    )
    early.start()
    lines = [
        jnp.broadcast_to(coef[m:m + 1, :], (SUB, lanes)) for m in range(2 * ITERS + 1)
    ]
    gain, res = lines[:ITERS], lines[ITERS:]
    copies = []
    for c in range(rows // chunk):
        @pl.loop(c * chunk, (c + 1) * chunk)
        def _(j):
            for t in range(tiles):
                at = pl.ds(t * SUB, SUB)
                base = [basis[k, j + 1, at, :] for k in range(ITERS + 1)]
                scale = lax.rsqrt(ds[j + 1, at, :])
                moved, left = gain[0] * base[0], res[0] * base[0]
                for k in range(1, ITERS + 1):
                    if k < ITERS:
                        moved = moved + gain[k] * base[k]
                    left = left + res[k] * base[k]
                next_ref[j, at, :] = xs[j + 1, at, :] + scale * moved
                residual_ref[j, at, :] = scale * left

        part = pl.ds(c * chunk, chunk)
        for i, (source, target) in enumerate([(next_ref, next_hbm), (residual_ref, residual_hbm)]):
            copies.append(pltpu.make_async_copy(source.at[part], target.at[part], sems.at[1 + i, c]))
            copies[-1].start()

    for j in range(done, rows):
        radiate(
            j, xs[j + 1], vapour_ref, cos_ref, albedo_ref, maskv, wcol, wide, scales,
            partial, rest,
        )
    late = pltpu.make_async_copy(
        rest.at[pl.ds(done, rows - done)], net_hbm.at[pl.ds(done, rows - done)], sems.at[0, 1]
    )
    late.start()
    for copy in [early] + copies + [late]:
        copy.wait()


def body(mesh_shape, state_prev, diffusivity, vapour, cos_zenith, albedo, absorption, solar_weight, day_mask):
    nx, ny = mesh_shape
    rows, levels, lanes = state_prev.shape
    gpoints = absorption.shape[1]
    weight = solar_weight[None, :]
    absorb = absorption.T
    vmem = pl.BlockSpec(memory_space=pltpu.VMEM)
    hbm = pl.BlockSpec(memory_space=pltpu.HBM)
    dma = pltpu.SemaphoreType.DMA
    kinds = ITERS + 2
    packs = 2 * rows * (levels // SUB) // lanes * SUB
    cells = (rows, levels, lanes)
    around = (rows + 2, levels, lanes)
    scales = pltpu.VMEM((2, levels, lanes), F32)
    partial = pltpu.VMEM((levels * SUB, lanes), F32)
    held = pl.pallas_call(
        functools.partial(solve_kernel, nx, ny),
        out_shape=[
            pltpu.VMEM((ITERS + 1,) + around, F32),
            pltpu.VMEM(around, F32),
            pltpu.VMEM(around, F32),
            pltpu.VMEM(cells, F32),
            pltpu.VMEM((rows, lanes), F32),
            pltpu.VMEM((rows, lanes), F32),
            pltpu.VMEM(cells, F32),
            pltpu.VMEM((levels, gpoints, lanes), F32),
            pltpu.VMEM((gpoints, lanes), F32),
            pltpu.VMEM((rows, lanes), F32),
            pltpu.VMEM((2 * SUB, lanes), F32),
        ],
        in_specs=[hbm] * 8,
        out_specs=[vmem] * 11,
        scratch_shapes=[
            pltpu.VMEM(around, F32),
            pltpu.VMEM(cells, F32),
            pltpu.VMEM(cells, F32),
            pltpu.VMEM(cells, F32),
            pltpu.VMEM((gpoints, levels), F32),
            pltpu.VMEM((1, gpoints), F32),
            pltpu.SMEM((rows,), jnp.int32),
            pltpu.VMEM((kinds, packs, lanes), F32),
            pltpu.VMEM((kinds, 2, packs, lanes), F32),
            pltpu.VMEM((2, packs, lanes), F32),
            scales,
            partial,
            pltpu.VMEM((2 * ITERS + 1, SUB, lanes), F32),
            pltpu.VMEM((2, 2 * SUB, lanes), F32),
            pltpu.VMEM((2, nx, 2 * SUB, lanes), F32),
            pltpu.VMEM((2, 2 * SUB, lanes), F32),
            pltpu.VMEM((2, ny, 2 * SUB, lanes), F32),
            dma((8,)),
            dma((kinds, 2)), dma((kinds, 2)), dma((kinds, 2)), dma((kinds, 2)),
            dma((2, nx)), dma((2, nx)), dma((2, ny)), dma((2, ny)),
        ],
        compiler_params=pltpu.CompilerParams(
            collective_id=0, has_side_effects=True, vmem_limit_bytes=16 * 1024 * 1024
        ),
    )(state_prev, diffusivity, vapour, cos_zenith, albedo, day_mask, absorb, weight)
    held = [pltpu.with_memory_space_constraint(h, pltpu.VMEM) for h in held]
    out = jax.ShapeDtypeStruct(cells, F32)
    return pl.pallas_call(
        finish_kernel,
        out_shape=(out, out, out),
        in_specs=[vmem] * 11,
        out_specs=(hbm, hbm, hbm),
        scratch_shapes=[
            pltpu.VMEM(cells, F32),
            pltpu.VMEM(cells, F32),
            pltpu.VMEM(cells, F32),
            scales,
            partial,
            dma((3, 4)),
        ],
        compiler_params=pltpu.CompilerParams(vmem_limit_bytes=8 * 1024 * 1024),
    )(*held)


def solution(mesh):
    cells = P("gy", None, "gx")
    columns = P("gy", "gx")
    return jax.shard_map(
        functools.partial(body, (mesh.shape["gx"], mesh.shape["gy"])),
        mesh=mesh,
        in_specs=(cells, cells, cells, columns, columns, P(), P(), P(("gx", "gy"))),
        out_specs=(cells, cells, cells),
        check_vma=False,
    )
```

```python
import functools
import math

import jax
import jax.numpy as jnp
from jax import lax
from jax.experimental import pallas as pl
from jax.experimental.pallas import tpu as pltpu
from jax.sharding import PartitionSpec as P

ITERS = 5
SUB = 8
WINDOWS = ITERS + 3
SHARES = (0, 1, 3, 5, 7, 9, 11, 13, 15)
UNROLL = 64
GROUP = 4
LOG2E = math.log2(math.e)
MESH = pl.DeviceIdType.MESH
F32 = jnp.float32


def edge(rows, w):
    return rows * SHARES[w] // 16


def radiate(j, state, vapour_ref, cos_ref, albedo_ref, maskv_ref, wcol_ref, wide, scales, partial, net_ref):
    levels, gpoints, lanes = wide.shape
    down_scale, up_scale = scales.at[0], scales.at[1]
    cosine = cos_ref[pl.ds(j, 1), :]
    optical = vapour_ref[j] * (1.0 + 0.5 * jnp.tanh(state))
    down_scale[...] = optical * (-LOG2E / cosine)
    up_scale[...] = optical * (-1.66 * LOG2E)

    def downward(l, carry):
        carry = carry * jnp.exp2(wide[l] * down_scale[pl.ds(l, 1), :])
        partial[pl.ds(pl.multiple_of(l * SUB, SUB), SUB), :] = jnp.sum(
            carry.reshape(gpoints // SUB, SUB, lanes), 0
        )
        return carry

    carry = lax.fori_loop(0, levels, downward, wcol_ref[...] * cosine, unroll=UNROLL)
    carry = carry * albedo_ref[pl.ds(j, 1), :]

    def upward(i, carry):
        l = levels - 1 - i
        where = pl.ds(pl.multiple_of(l * SUB, SUB), SUB)
        partial[where, :] = partial[where, :] - jnp.sum(
            carry.reshape(gpoints // SUB, SUB, lanes), 0
        )
        return carry * jnp.exp2(wide[l] * up_scale[pl.ds(l, 1), :])

    lax.fori_loop(0, levels, upward, carry, unroll=UNROLL)
    total = partial[pl.ds(0, levels, stride=SUB), :]
    for s in range(1, SUB):
        total = total + partial[pl.ds(s, levels, stride=SUB), :]
    net_ref[j] = total * maskv_ref[pl.ds(j, 1), :]


def solve_kernel(
    nx, ny,
    state_hbm, diff_hbm, vapour_hbm, cos_hbm, albedo_hbm, mask_hbm, absorb_hbm, weight_hbm,
    basis, state_ref, ds, vapour_ref, cos_ref, albedo_ref, net_ref, wide, wcol, maskv, coef,
    xs, diff_ref, root, degree, gain_d, inverse_d, absorb, weight_row, mask_smem,
    lon_send, lon_recv, lon_root, scales, partial, sums, mine, stage_one, half_sum, stage_two,
    in_sem, lat_ssem, lat_rsem, lon_ssem, lon_rsem, one_ssem, one_rsem, two_ssem, two_rsem,
):
    rows, levels, lanes = vapour_ref.shape
    gpoints = wide.shape[1]
    tiles = lanes // SUB
    per = GROUP
    groups = rows // per
    moments = 2 * ITERS + 1
    ix = lax.axis_index("gx")
    iy = lax.axis_index("gy")
    gx_east, gx_west = lax.rem(ix + 1, nx), lax.rem(ix + nx - 1, nx)

    loads = [
        pltpu.make_async_copy(src, dst, in_sem.at[i])
        for i, (src, dst) in enumerate([
            (diff_hbm, diff_ref), (state_hbm, state_ref), (absorb_hbm, absorb),
            (weight_hbm, weight_row), (mask_hbm, mask_smem), (cos_hbm, cos_ref),
            (albedo_hbm, albedo_ref), (vapour_hbm, vapour_ref),
        ])
    ]
    for load in loads:
        load.start()

    barrier = pltpu.get_barrier_semaphore()
    for d in range(1, nx):
        pl.semaphore_signal(
            barrier, inc=1, device_id=(lax.rem(ix + d, nx), iy), device_id_type=MESH
        )
    for d in range(1, ny):
        pl.semaphore_signal(
            barrier, inc=1, device_id=(ix, lax.rem(iy + d, ny)), device_id_type=MESH
        )

    lane = lax.broadcasted_iota(jnp.int32, (SUB, levels), 1)
    sub = lax.broadcasted_iota(jnp.int32, (SUB, levels), 0)
    first_lane, last_lane = lane == 0, lane == levels - 1
    first_sub, last_sub = sub == 0, sub == SUB - 1
    zero = jnp.zeros((SUB, levels), F32)

    def field(k):
        return ds if k == 0 else xs if k == 1 else basis.at[k - 2]

    def lat_copy(k, side):
        ref = field(k) if isinstance(k, int) else basis.at[k - 2]
        return pltpu.make_async_remote_copy(
            src_ref=ref.at[1 if side == 0 else rows],
            dst_ref=ref.at[rows + 1 if side == 0 else 0],
            send_sem=lat_ssem.at[k, side],
            recv_sem=lat_rsem.at[k, side],
            device_id=(ix, lax.rem(iy + ny - 1, ny) if side == 0 else lax.rem(iy + 1, ny)),
            device_id_type=MESH,
        )

    def lon_copy(k, side):
        return pltpu.make_async_remote_copy(
            src_ref=lon_send.at[k, side],
            dst_ref=lon_recv.at[k, side],
            send_sem=lon_ssem.at[k, side],
            recv_sem=lon_rsem.at[k, side],
            device_id=(gx_west if side == 0 else gx_east, iy),
            device_id_type=MESH,
        )

    def send_halo(k):
        @pl.when(iy > 0)
        def _():
            lat_copy(k, 0).start()

        @pl.when(iy < ny - 1)
        def _():
            lat_copy(k, 1).start()

        for side in range(2):
            lon_copy(k, side).start()

    def wait_halo(k):
        @pl.when(iy > 0)
        def _():
            lat_copy(k, 0).wait_send()
            lat_copy(k, 1).wait_recv()

        @pl.when(iy < ny - 1)
        def _():
            lat_copy(k, 1).wait_send()
            lat_copy(k, 0).wait_recv()

        for side in range(2):
            lon_copy(k, side).wait()

    def edges(k, j, values):
        lon_send[k, 0, pl.ds(j, 1), :] = values[0][0:1, :]
        lon_send[k, 1, pl.ds(j, 1), :] = values[-1][-1:, :]

    def level_pair(value):
        return (
            jnp.where(last_lane, 0.0, pltpu.roll(value, levels - 1, 1)),
            jnp.where(first_lane, 0.0, pltpu.roll(value, 1, 1)),
        )

    def lon_pair(values, halo, j):
        later = [pltpu.roll(v, 1, 0) for v in values]
        sooner = [pltpu.roll(v, SUB - 1, 0) for v in values]
        west, east = halo[1, pl.ds(j, 1), :], halo[0, pl.ds(j, 1), :]
        at_west = [
            jnp.where(first_sub, later[t - 1] if t else west, later[t]) for t in range(tiles)
        ]
        at_east = [
            jnp.where(last_sub, sooner[t + 1] if t < tiles - 1 else east, sooner[t])
            for t in range(tiles)
        ]
        return at_west, at_east

    def plane_of(ref, j):
        return [ref[j, t * SUB:(t + 1) * SUB, :] for t in range(tiles)]

    def reduce_copy(r, stage, d):
        buffer = stage_one if stage == 0 else stage_two
        slot = ix if stage == 0 else iy
        ssem = one_ssem if stage == 0 else two_ssem
        rsem = one_rsem if stage == 0 else two_rsem
        peer = (lax.rem(ix + d, nx), iy) if stage == 0 else (ix, lax.rem(iy + d, ny))
        return pltpu.make_async_remote_copy(
            src_ref=(mine if stage == 0 else half_sum).at[r],
            dst_ref=buffer.at[r, slot],
            send_sem=ssem.at[r, d - 1],
            recv_sem=rsem.at[r, d - 1],
            device_id=peer,
            device_id_type=MESH,
        )

    def reduce_start(r, stage):
        source, buffer = (mine, stage_one) if stage == 0 else (half_sum, stage_two)
        n = nx if stage == 0 else ny
        buffer[r, ix if stage == 0 else iy] = source[r]
        for d in range(1, n):
            reduce_copy(r, stage, d).start()

    def reduce_end(r, stage):
        n = nx if stage == 0 else ny
        for d in range(1, n):
            reduce_copy(r, stage, d).wait()
        buffer = stage_one if stage == 0 else stage_two
        total = buffer[r, 0]
        for d in range(1, n):
            total = total + buffer[r, d]
        return total

    def all_lanes(values):
        return jnp.broadcast_to(jnp.sum(values, 1, keepdims=True), values.shape)

    def window(first, last):
        @pl.loop(first, last)
        def _(j):
            radiate(
                j, state_ref[j], vapour_ref, cos_ref, albedo_ref, maskv, wcol, wide, scales,
                partial, net_ref,
            )

    for k in range(2, 2 + ITERS):
        @pl.when(iy == 0)
        def _():
            basis[k - 2, 0] = jnp.zeros((lanes, levels), F32)

        @pl.when(iy == ny - 1)
        def _():
            basis[k - 2, rows + 1] = jnp.zeros((lanes, levels), F32)

    for k in range(2):
        loads[k].wait()

        given = diff_ref if k == 0 else state_ref

        @pl.loop(0, rows, unroll=4)
        def _(j):
            turned = given[j].T
            field(k)[j + 1] = turned
            edges(k, j, [turned])

    pl.semaphore_wait(barrier, nx + ny - 2)
    for k in range(2):
        send_halo(k)

    def spread(j, total):
        part = zero
        for t in range(tiles):
            here = pl.ds(t * SUB, SUB)
            d = ds[j + 1, here, :]
            reciprocal = lax.rsqrt(d)
            root[j + 1, here, :] = d * reciprocal
            inverse_d[j, here, :] = reciprocal * reciprocal
            square = d * d
            part = part + square * square * square
        return total + part

    squares = lax.fori_loop(0, rows, spread, zero)
    mine[0] = jnp.concatenate([squares, jnp.zeros_like(squares)], 0)
    reduce_start(0, 0)

    for load in loads[2:]:
        load.wait()

    for j in range(rows):
        maskv[j:j + 1, :] = jnp.full((1, lanes), mask_smem[j].astype(F32), F32)
    column = jnp.broadcast_to(weight_row[...], (lanes, gpoints)).T
    wcol[...] = column

    spans = 4

    @pl.loop(0, spans)
    def _(i):
        span = levels // spans
        turned = pltpu.roll(absorb[...], lax.rem(levels - i * span, levels), 1)
        for m in range(span):
            wide[i * span + m] = jnp.broadcast_to(turned[:, m:m + 1], (gpoints, lanes))

    window(0, edge(rows, 1))
    half_sum[0] = reduce_end(0, 0)
    reduce_start(0, 1)

    wait_halo(0)
    wait_halo(1)

    @pl.when(iy > 0)
    def _():
        root[0] = ds[0] * lax.rsqrt(ds[0])

    @pl.when(iy == 0)
    def _():
        root[0] = jnp.zeros((lanes, levels), F32)
        xs[0] = jnp.zeros((lanes, levels), F32)

    @pl.when(iy < ny - 1)
    def _():
        root[rows + 1] = ds[rows + 1] * lax.rsqrt(ds[rows + 1])

    @pl.when(iy == ny - 1)
    def _():
        root[rows + 1] = jnp.zeros((lanes, levels), F32)
        xs[rows + 1] = jnp.zeros((lanes, levels), F32)

    for side in range(2):
        d = lon_recv[0, side]
        lon_root[side] = d * lax.rsqrt(d)

    @pl.loop(0, groups)
    def _(g):
        for i in range(per):
            j = g * per + i
            s_here, x_here = plane_of(root, j + 1), plane_of(xs, j + 1)
            s_west, s_east = lon_pair(s_here, lon_root, j)
            x_west, x_east = lon_pair(x_here, lon_recv.at[1], j)
            started = []
            for t in range(tiles):
                at = pl.ds(t * SUB, SUB)
                s_pairs = level_pair(s_here[t]) + (
                    root[j + 2, at, :], root[j, at, :], s_west[t], s_east[t]
                )
                x_pairs = level_pair(x_here[t]) + (
                    xs[j + 2, at, :], xs[j, at, :], x_west[t], x_east[t]
                )
                around, change = None, None
                for s, x in zip(s_pairs, x_pairs):
                    term = s * (x - x_here[t])
                    around = s if around is None else around + s
                    change = term if change is None else change + term
                degree[j, at, :] = s_here[t] * around
                start = ds[j + 1, at, :] * change
                basis[0, j + 1, at, :] = start
                started.append(start)
            edges(2, j, started)

    send_halo(2)
    window(edge(rows, 1), edge(rows, 2))
    squares = reduce_end(0, 1)
    count = nx * ny * rows * levels * lanes
    squares = all_lanes(jnp.sum(squares, 0, keepdims=True))
    half = 6.0 * jnp.exp(jnp.log(squares * (1.0 / count)) * (1.0 / 6.0))
    twice = jnp.broadcast_to(2.0 / half, (SUB, levels))

    def advance(k, first, last):
        wait_halo(2 + k)
        halo = lon_recv.at[2 + k]
        here, there = basis.at[k], basis.at[k + 1]

        def step(g, totals):
            parts = [zero] * len(totals)
            for i in range(per):
                j = g * per + i
                u = plane_of(here, j + 1)
                west, east = lon_pair(u, halo, j)
                latest = []
                for t in range(tiles):
                    at = pl.ds(t * SUB, SUB)
                    below, above = level_pair(u[t])
                    around = ((east[t] + west[t]) + (above + below)) + (
                        here[j + 2, at, :] + here[j, at, :]
                    )
                    if first:
                        own = twice * degree[j, at, :] - 2.0
                        other = twice * ds[j + 1, at, :]
                        degree[j, at, :] = own
                        gain_d[j, at, :] = other
                        later = 0.5 * (own * u[t] - other * around)
                    else:
                        later = degree[j, at, :] * u[t] - gain_d[j, at, :] * around
                        later = later - basis[k - 1, j + 1, at, :]
                    there[j + 1, at, :] = later
                    weighed = later * inverse_d[j, at, :]
                    parts[0] = parts[0] + weighed * u[t]
                    parts[1] = parts[1] + weighed * later
                    if first:
                        parts[2] = parts[2] + (u[t] * inverse_d[j, at, :]) * u[t]
                    latest.append(later)
                if not last:
                    edges(3 + k, j, latest)
            return tuple(a + b for a, b in zip(totals, parts))

        totals = lax.fori_loop(0, groups, step, (zero,) * (3 if first else 2))
        sums[2 * k + 1] = totals[0]
        sums[2 * k + 2] = totals[1]
        if first:
            sums[0] = totals[2]

    for k in range(ITERS):
        advance(k, k == 0, k == ITERS - 1)
        if k < ITERS - 1:
            send_halo(3 + k)
            window(edge(rows, 2 + k), edge(rows, 3 + k))

    lines = [jnp.sum(sums[m], 0, keepdims=True) for m in range(moments)]
    lines += [jnp.zeros_like(lines[0])] * (2 * SUB - moments)
    mine[1] = jnp.concatenate(lines, 0)
    reduce_start(1, 0)
    window(edge(rows, ITERS + 1), edge(rows, ITERS + 2))
    half_sum[1] = reduce_end(1, 0)
    reduce_start(1, 1)
    window(edge(rows, ITERS + 2), edge(rows, ITERS + 3))
    values = all_lanes(reduce_end(1, 1))
    raw = [values[m:m + 1, :] for m in range(moments)]

    mu = [raw[0], raw[1]]
    for k in range(1, ITERS + 1):
        mu.append(2.0 * raw[2 * k] - mu[0])
        if k < ITERS:
            mu.append(2.0 * raw[2 * k + 1] - mu[1])
    gram = [
        [0.5 * (mu[i + j] + mu[abs(i - j)]) for j in range(ITERS + 1)] for i in range(ITERS + 1)
    ]

    def inner(a, b):
        terms = []
        for i in range(len(a)):
            for j in range(len(b)):
                terms.append((a[i] * b[j]) * gram[i][j])
        while len(terms) > 1:
            terms = [
                terms[i] + terms[i + 1] if i + 1 < len(terms) else terms[i]
                for i in range(0, len(terms), 2)
            ]
        return terms[0]

    centre = half + 1.0
    one = jnp.ones_like(half)
    none = jnp.zeros_like(half)
    res, direction, gain = [one], [one], [none] * ITERS
    current = inner(res, res)
    for iteration in range(ITERS):
        image = [centre * c for c in direction] + [none]
        for j, c in enumerate(direction):
            if j == 0:
                image[1] = image[1] + half * c
            else:
                image[j + 1] = image[j + 1] + 0.5 * half * c
                image[j - 1] = image[j - 1] + 0.5 * half * c
        step = current / inner(direction, image)
        for j, c in enumerate(direction):
            gain[j] = gain[j] + step * c
        res = [r - step * q for r, q in zip(res + [none], image)]
        if iteration < ITERS - 1:
            following = inner(res, res)
            ratio = following / current
            direction = [r + ratio * c for r, c in zip(res, direction + [none])]
            current = following

    lines = gain + res
    lines += [none] * (2 * SUB - len(lines))
    coef[...] = jnp.concatenate(lines, 0)


def finish_kernel(
    basis, state_ref, ds, vapour_ref, cos_ref, albedo_ref, net_ref, wide, wcol, maskv, coef,
    next_hbm, residual_hbm, net_hbm,
    next_ref, residual_ref, rest, scales, partial, sems,
):
    rows = vapour_ref.shape[0]
    done = edge(rows, WINDOWS)
    chunk = rows // 4
    early = pltpu.make_async_copy(
        net_ref.at[pl.ds(0, done)], net_hbm.at[pl.ds(0, done)], sems.at[0, 0]
    )
    early.start()
    lines = [coef[m:m + 1, :] for m in range(2 * ITERS + 1)]
    gain, res = lines[:ITERS], lines[ITERS:]
    copies = []
    for c in range(rows // chunk):
        @pl.loop(c * chunk, (c + 1) * chunk, unroll=chunk)
        def _(j):
            base = [basis[k, j + 1] for k in range(ITERS + 1)]
            scale = lax.rsqrt(ds[j + 1])
            moved, left = gain[0] * base[0], res[0] * base[0]
            for k in range(1, ITERS + 1):
                if k < ITERS:
                    moved = moved + gain[k] * base[k]
                left = left + res[k] * base[k]
            next_ref[j] = state_ref[j] + (scale * moved).T
            residual_ref[j] = (scale * left).T

        part = pl.ds(c * chunk, chunk)
        for i, (source, target) in enumerate([(next_ref, next_hbm), (residual_ref, residual_hbm)]):
            copies.append(pltpu.make_async_copy(source.at[part], target.at[part], sems.at[1 + i, c]))
            copies[-1].start()

    for j in range(done, rows):
        radiate(
            j, state_ref[j], vapour_ref, cos_ref, albedo_ref, maskv, wcol, wide, scales,
            partial, rest,
        )
    late = pltpu.make_async_copy(
        rest.at[pl.ds(done, rows - done)], net_hbm.at[pl.ds(done, rows - done)], sems.at[0, 1]
    )
    late.start()
    for copy in [early] + copies + [late]:
        copy.wait()


def body(mesh_shape, state_prev, diffusivity, vapour, cos_zenith, albedo, absorption, solar_weight, day_mask):
    nx, ny = mesh_shape
    rows, levels, lanes = state_prev.shape
    gpoints = absorption.shape[1]
    weight = solar_weight[None, :]
    absorb = absorption.T
    vmem = pl.BlockSpec(memory_space=pltpu.VMEM)
    hbm = pl.BlockSpec(memory_space=pltpu.HBM)
    dma = pltpu.SemaphoreType.DMA
    kinds = ITERS + 2
    cells = (rows, levels, lanes)
    turned = (rows, lanes, levels)
    around = (rows + 2, lanes, levels)
    scales = pltpu.VMEM((2, levels, lanes), F32)
    partial = pltpu.VMEM((levels * SUB, lanes), F32)
    held = pl.pallas_call(
        functools.partial(solve_kernel, nx, ny),
        out_shape=[
            pltpu.VMEM((ITERS + 1,) + around, F32),
            pltpu.VMEM(cells, F32),
            pltpu.VMEM(around, F32),
            pltpu.VMEM(cells, F32),
            pltpu.VMEM((rows, lanes), F32),
            pltpu.VMEM((rows, lanes), F32),
            pltpu.VMEM(cells, F32),
            pltpu.VMEM((levels, gpoints, lanes), F32),
            pltpu.VMEM((gpoints, lanes), F32),
            pltpu.VMEM((rows, lanes), F32),
            pltpu.VMEM((2 * SUB, levels), F32),
        ],
        in_specs=[hbm] * 8,
        out_specs=[vmem] * 11,
        scratch_shapes=[
            pltpu.VMEM(around, F32),
            pltpu.VMEM(cells, F32),
            pltpu.VMEM(around, F32),
            pltpu.VMEM(turned, F32),
            pltpu.VMEM(turned, F32),
            pltpu.VMEM(turned, F32),
            pltpu.VMEM((gpoints, levels), F32),
            pltpu.VMEM((1, gpoints), F32),
            pltpu.SMEM((rows,), jnp.int32),
            pltpu.VMEM((kinds, 2, rows, levels), F32),
            pltpu.VMEM((kinds, 2, rows, levels), F32),
            pltpu.VMEM((2, rows, levels), F32),
            scales,
            partial,
            pltpu.VMEM((2 * ITERS + 1, SUB, levels), F32),
            pltpu.VMEM((2, 2 * SUB, levels), F32),
            pltpu.VMEM((2, nx, 2 * SUB, levels), F32),
            pltpu.VMEM((2, 2 * SUB, levels), F32),
            pltpu.VMEM((2, ny, 2 * SUB, levels), F32),
            dma((8,)),
            dma((kinds, 2)), dma((kinds, 2)), dma((kinds, 2)), dma((kinds, 2)),
            dma((2, nx)), dma((2, nx)), dma((2, ny)), dma((2, ny)),
        ],
        compiler_params=pltpu.CompilerParams(
            collective_id=0, has_side_effects=True, vmem_limit_bytes=18 * 1024 * 1024
        ),
    )(*[
        pltpu.with_memory_space_constraint(a, pltpu.HBM)
        for a in (state_prev, diffusivity, vapour, cos_zenith, albedo, day_mask, absorb, weight)
    ])
    held = [pltpu.with_memory_space_constraint(h, pltpu.VMEM) for h in held]
    out = jax.ShapeDtypeStruct(cells, F32)
    return pl.pallas_call(
        finish_kernel,
        out_shape=(out, out, out),
        in_specs=[vmem] * 11,
        out_specs=(hbm, hbm, hbm),
        scratch_shapes=[
            pltpu.VMEM(cells, F32),
            pltpu.VMEM(cells, F32),
            pltpu.VMEM(cells, F32),
            scales,
            partial,
            dma((3, 4)),
        ],
        compiler_params=pltpu.CompilerParams(vmem_limit_bytes=8 * 1024 * 1024),
    )(*held)


def solution(mesh):
    cells = P("gy", None, "gx")
    columns = P("gy", "gx")
    return jax.shard_map(
        functools.partial(body, (mesh.shape["gx"], mesh.shape["gy"])),
        mesh=mesh,
        in_specs=(cells, cells, cells, columns, columns, P(), P(), P(("gx", "gy"))),
        out_specs=(cells, cells, cells),
        check_vma=False,
    )
```

```python
import functools
import math

import jax
import jax.numpy as jnp
from jax import lax
from jax.experimental import pallas as pl
from jax.experimental.pallas import tpu as pltpu
from jax.sharding import PartitionSpec as P

ITERS = 5
SUB = 8
WINDOWS = ITERS + 3
SHARES = (0, 1, 3, 5, 7, 9, 11, 13, 15)
UNROLL = 64
GROUP = 4
LOG2E = math.log2(math.e)
MESH = pl.DeviceIdType.MESH
F32 = jnp.float32


def edge(rows, w):
    return rows * SHARES[w] // 16


def radiate(j, state, vapour_ref, cos_ref, albedo_ref, maskv_ref, wcol_ref, wide, scales, partial, net_ref):
    levels, gpoints, lanes = wide.shape
    down_scale, up_scale = scales.at[0], scales.at[1]
    cosine = cos_ref[pl.ds(j, 1), :]
    optical = vapour_ref[j] * (1.0 + 0.5 * jnp.tanh(state))
    down_scale[...] = optical * (-LOG2E / cosine)
    up_scale[...] = optical * (-1.66 * LOG2E)

    def downward(l, carry):
        carry = carry * jnp.exp2(wide[l] * down_scale[pl.ds(l, 1), :])
        partial[pl.ds(pl.multiple_of(l * SUB, SUB), SUB), :] = jnp.sum(
            carry.reshape(gpoints // SUB, SUB, lanes), 0
        )
        return carry

    carry = lax.fori_loop(0, levels, downward, wcol_ref[...] * cosine, unroll=UNROLL)
    carry = carry * albedo_ref[pl.ds(j, 1), :]

    def upward(i, carry):
        l = levels - 1 - i
        where = pl.ds(pl.multiple_of(l * SUB, SUB), SUB)
        partial[where, :] = partial[where, :] - jnp.sum(
            carry.reshape(gpoints // SUB, SUB, lanes), 0
        )
        return carry * jnp.exp2(wide[l] * up_scale[pl.ds(l, 1), :])

    lax.fori_loop(0, levels, upward, carry, unroll=UNROLL)
    total = partial[pl.ds(0, levels, stride=SUB), :]
    for s in range(1, SUB):
        total = total + partial[pl.ds(s, levels, stride=SUB), :]
    net_ref[j] = total * maskv_ref[pl.ds(j, 1), :]


def solve_kernel(
    nx, ny,
    state_hbm, diff_hbm, vapour_hbm, cos_hbm, albedo_hbm, mask_hbm, absorb_hbm, weight_hbm,
    basis, state_ref, ds, vapour_ref, cos_ref, albedo_ref, net_ref, wide, wcol, maskv, coef,
    xs, diff_ref, root, degree, gain_d, inverse_d, absorb, weight_row, mask_smem,
    lon_send, lon_recv, lon_root, scales, partial, sums, mine, stage_one, half_sum, stage_two,
    in_sem, lat_ssem, lat_rsem, lon_ssem, lon_rsem, one_ssem, one_rsem, two_ssem, two_rsem,
):
    rows, levels, lanes = vapour_ref.shape
    gpoints = wide.shape[1]
    tiles = lanes // SUB
    per = GROUP
    groups = rows // per
    moments = 2 * ITERS + 1
    ix = lax.axis_index("gx")
    iy = lax.axis_index("gy")
    gx_east, gx_west = lax.rem(ix + 1, nx), lax.rem(ix + nx - 1, nx)

    loads = [
        pltpu.make_async_copy(src, dst, in_sem.at[i])
        for i, (src, dst) in enumerate([
            (diff_hbm, diff_ref), (state_hbm, state_ref), (absorb_hbm, absorb),
            (weight_hbm, weight_row), (mask_hbm, mask_smem), (cos_hbm, cos_ref),
            (albedo_hbm, albedo_ref), (vapour_hbm, vapour_ref),
        ])
    ]
    for load in loads:
        load.start()

    barrier = pltpu.get_barrier_semaphore()
    for d in range(1, nx):
        pl.semaphore_signal(
            barrier, inc=1, device_id=(lax.rem(ix + d, nx), iy), device_id_type=MESH
        )
    for d in range(1, ny):
        pl.semaphore_signal(
            barrier, inc=1, device_id=(ix, lax.rem(iy + d, ny)), device_id_type=MESH
        )

    lane = lax.broadcasted_iota(jnp.int32, (SUB, levels), 1)
    sub = lax.broadcasted_iota(jnp.int32, (SUB, levels), 0)
    first_lane, last_lane = lane == 0, lane == levels - 1
    first_sub, last_sub = sub == 0, sub == SUB - 1
    zero = jnp.zeros((SUB, levels), F32)

    def field(k):
        return ds if k == 0 else xs if k == 1 else basis.at[k - 2]

    def lat_copy(k, side):
        ref = field(k) if isinstance(k, int) else basis.at[k - 2]
        return pltpu.make_async_remote_copy(
            src_ref=ref.at[1 if side == 0 else rows],
            dst_ref=ref.at[rows + 1 if side == 0 else 0],
            send_sem=lat_ssem.at[k, side],
            recv_sem=lat_rsem.at[k, side],
            device_id=(ix, lax.rem(iy + ny - 1, ny) if side == 0 else lax.rem(iy + 1, ny)),
            device_id_type=MESH,
        )

    def lon_copy(k, side):
        return pltpu.make_async_remote_copy(
            src_ref=lon_send.at[k, side],
            dst_ref=lon_recv.at[k, side],
            send_sem=lon_ssem.at[k, side],
            recv_sem=lon_rsem.at[k, side],
            device_id=(gx_west if side == 0 else gx_east, iy),
            device_id_type=MESH,
        )

    def send_halo(k):
        @pl.when(iy > 0)
        def _():
            lat_copy(k, 0).start()

        @pl.when(iy < ny - 1)
        def _():
            lat_copy(k, 1).start()

        for side in range(2):
            lon_copy(k, side).start()

    def wait_halo(k):
        @pl.when(iy > 0)
        def _():
            lat_copy(k, 0).wait_send()
            lat_copy(k, 1).wait_recv()

        @pl.when(iy < ny - 1)
        def _():
            lat_copy(k, 1).wait_send()
            lat_copy(k, 0).wait_recv()

        for side in range(2):
            lon_copy(k, side).wait()

    def edges(k, j, values):
        lon_send[k, 0, pl.ds(j, 1), :] = values[0][0:1, :]
        lon_send[k, 1, pl.ds(j, 1), :] = values[-1][-1:, :]

    def level_pair(value):
        return (
            jnp.where(last_lane, 0.0, pltpu.roll(value, levels - 1, 1)),
            jnp.where(first_lane, 0.0, pltpu.roll(value, 1, 1)),
        )

    def lon_pair(values, halo, j):
        later = [pltpu.roll(v, 1, 0) for v in values]
        sooner = [pltpu.roll(v, SUB - 1, 0) for v in values]
        west, east = halo[1, pl.ds(j, 1), :], halo[0, pl.ds(j, 1), :]
        at_west = [
            jnp.where(first_sub, later[t - 1] if t else west, later[t]) for t in range(tiles)
        ]
        at_east = [
            jnp.where(last_sub, sooner[t + 1] if t < tiles - 1 else east, sooner[t])
            for t in range(tiles)
        ]
        return at_west, at_east

    def plane_of(ref, j):
        return [ref[j, t * SUB:(t + 1) * SUB, :] for t in range(tiles)]

    def reduce_copy(r, stage, d):
        buffer = stage_one if stage == 0 else stage_two
        slot = ix if stage == 0 else iy
        ssem = one_ssem if stage == 0 else two_ssem
        rsem = one_rsem if stage == 0 else two_rsem
        peer = (lax.rem(ix + d, nx), iy) if stage == 0 else (ix, lax.rem(iy + d, ny))
        return pltpu.make_async_remote_copy(
            src_ref=(mine if stage == 0 else half_sum).at[r],
            dst_ref=buffer.at[r, slot],
            send_sem=ssem.at[r, d - 1],
            recv_sem=rsem.at[r, d - 1],
            device_id=peer,
            device_id_type=MESH,
        )

    def reduce_start(r, stage):
        source, buffer = (mine, stage_one) if stage == 0 else (half_sum, stage_two)
        n = nx if stage == 0 else ny
        buffer[r, ix if stage == 0 else iy] = source[r]
        for d in range(1, n):
            reduce_copy(r, stage, d).start()

    def reduce_end(r, stage):
        n = nx if stage == 0 else ny
        for d in range(1, n):
            reduce_copy(r, stage, d).wait()
        buffer = stage_one if stage == 0 else stage_two
        total = buffer[r, 0]
        for d in range(1, n):
            total = total + buffer[r, d]
        return total

    def all_lanes(values):
        return jnp.broadcast_to(jnp.sum(values, 1, keepdims=True), values.shape)

    def window(first, last):
        @pl.loop(first, last)
        def _(j):
            radiate(
                j, state_ref[j], vapour_ref, cos_ref, albedo_ref, maskv, wcol, wide, scales,
                partial, net_ref,
            )

    for k in range(2, 2 + ITERS):
        @pl.when(iy == 0)
        def _():
            basis[k - 2, 0] = jnp.zeros((lanes, levels), F32)

        @pl.when(iy == ny - 1)
        def _():
            basis[k - 2, rows + 1] = jnp.zeros((lanes, levels), F32)

    loads[0].wait()

    def spread(j, total):
        turned = diff_ref[j].T
        ds[j + 1] = turned
        edges(0, j, [turned])
        reciprocal = lax.rsqrt(turned)
        root[j + 1] = turned * reciprocal
        inverse_d[j] = reciprocal * reciprocal
        square = turned * turned
        return total + jnp.sum((square * square * square).reshape(tiles, SUB, levels), 0)

    squares = lax.fori_loop(0, rows, spread, zero, unroll=4)
    loads[1].wait()

    @pl.loop(0, rows, unroll=4)
    def _(j):
        turned = state_ref[j].T
        xs[j + 1] = turned
        edges(1, j, [turned])

    pl.semaphore_wait(barrier, nx + ny - 2)
    for k in range(2):
        send_halo(k)

    mine[0] = jnp.concatenate([squares, jnp.zeros_like(squares)], 0)
    reduce_start(0, 0)

    for load in loads[2:]:
        load.wait()

    for j in range(rows):
        maskv[j:j + 1, :] = jnp.full((1, lanes), mask_smem[j].astype(F32), F32)
    column = jnp.broadcast_to(weight_row[...], (lanes, gpoints)).T
    wcol[...] = column

    spans = 4

    @pl.loop(0, spans)
    def _(i):
        span = levels // spans
        turned = pltpu.roll(absorb[...], lax.rem(levels - i * span, levels), 1)
        for m in range(span):
            wide[i * span + m] = jnp.broadcast_to(turned[:, m:m + 1], (gpoints, lanes))

    window(0, edge(rows, 1))
    half_sum[0] = reduce_end(0, 0)
    reduce_start(0, 1)

    wait_halo(0)
    wait_halo(1)

    @pl.when(iy > 0)
    def _():
        root[0] = ds[0] * lax.rsqrt(ds[0])

    @pl.when(iy == 0)
    def _():
        root[0] = jnp.zeros((lanes, levels), F32)
        xs[0] = jnp.zeros((lanes, levels), F32)

    @pl.when(iy < ny - 1)
    def _():
        root[rows + 1] = ds[rows + 1] * lax.rsqrt(ds[rows + 1])

    @pl.when(iy == ny - 1)
    def _():
        root[rows + 1] = jnp.zeros((lanes, levels), F32)
        xs[rows + 1] = jnp.zeros((lanes, levels), F32)

    for side in range(2):
        d = lon_recv[0, side]
        lon_root[side] = d * lax.rsqrt(d)

    @pl.loop(0, groups)
    def _(g):
        for i in range(per):
            j = g * per + i
            s_here, x_here = plane_of(root, j + 1), plane_of(xs, j + 1)
            s_west, s_east = lon_pair(s_here, lon_root, j)
            x_west, x_east = lon_pair(x_here, lon_recv.at[1], j)
            started = []
            for t in range(tiles):
                at = pl.ds(t * SUB, SUB)
                s_pairs = level_pair(s_here[t]) + (
                    root[j + 2, at, :], root[j, at, :], s_west[t], s_east[t]
                )
                x_pairs = level_pair(x_here[t]) + (
                    xs[j + 2, at, :], xs[j, at, :], x_west[t], x_east[t]
                )
                around, change = None, None
                for s, x in zip(s_pairs, x_pairs):
                    term = s * (x - x_here[t])
                    around = s if around is None else around + s
                    change = term if change is None else change + term
                degree[j, at, :] = s_here[t] * around
                start = ds[j + 1, at, :] * change
                basis[0, j + 1, at, :] = start
                started.append(start)
            edges(2, j, started)

    send_halo(2)
    window(edge(rows, 1), edge(rows, 2))
    squares = reduce_end(0, 1)
    count = nx * ny * rows * levels * lanes
    squares = all_lanes(jnp.sum(squares, 0, keepdims=True))
    half = 6.0 * jnp.exp(jnp.log(squares * (1.0 / count)) * (1.0 / 6.0))
    twice = jnp.broadcast_to(2.0 / half, (SUB, levels))

    def advance(k, first, last):
        wait_halo(2 + k)
        halo = lon_recv.at[2 + k]
        here, there = basis.at[k], basis.at[k + 1]

        def step(g, totals):
            parts = [zero] * len(totals)
            for i in range(per):
                j = g * per + i
                u = plane_of(here, j + 1)
                west, east = lon_pair(u, halo, j)
                latest = []
                for t in range(tiles):
                    at = pl.ds(t * SUB, SUB)
                    below, above = level_pair(u[t])
                    around = ((east[t] + west[t]) + (above + below)) + (
                        here[j + 2, at, :] + here[j, at, :]
                    )
                    if first:
                        own = twice * degree[j, at, :] - 2.0
                        other = twice * ds[j + 1, at, :]
                        degree[j, at, :] = own
                        gain_d[j, at, :] = other
                        later = 0.5 * (own * u[t] - other * around)
                    else:
                        later = degree[j, at, :] * u[t] - gain_d[j, at, :] * around
                        later = later - basis[k - 1, j + 1, at, :]
                    there[j + 1, at, :] = later
                    weighed = later * inverse_d[j, at, :]
                    parts[0] = parts[0] + weighed * u[t]
                    parts[1] = parts[1] + weighed * later
                    if first:
                        parts[2] = parts[2] + (u[t] * inverse_d[j, at, :]) * u[t]
                    latest.append(later)
                if not last:
                    edges(3 + k, j, latest)
            return tuple(a + b for a, b in zip(totals, parts))

        totals = lax.fori_loop(0, groups, step, (zero,) * (3 if first else 2))
        sums[2 * k + 1] = totals[0]
        sums[2 * k + 2] = totals[1]
        if first:
            sums[0] = totals[2]

    for k in range(ITERS):
        advance(k, k == 0, k == ITERS - 1)
        if k < ITERS - 1:
            send_halo(3 + k)
            window(edge(rows, 2 + k), edge(rows, 3 + k))

    lines = [jnp.sum(sums[m], 0, keepdims=True) for m in range(moments)]
    lines += [jnp.zeros_like(lines[0])] * (2 * SUB - moments)
    mine[1] = jnp.concatenate(lines, 0)
    reduce_start(1, 0)
    window(edge(rows, ITERS + 1), edge(rows, ITERS + 2))
    half_sum[1] = reduce_end(1, 0)
    reduce_start(1, 1)
    window(edge(rows, ITERS + 2), edge(rows, ITERS + 3))
    values = reduce_end(1, 1)
    raw = [values[m:m + 1, :] for m in range(moments)]

    mu = [raw[0], raw[1]]
    for k in range(1, ITERS + 1):
        mu.append(2.0 * raw[2 * k] - mu[0])
        if k < ITERS:
            mu.append(2.0 * raw[2 * k + 1] - mu[1])
    gram = [
        [0.5 * (mu[i + j] + mu[abs(i - j)]) for j in range(ITERS + 1)] for i in range(ITERS + 1)
    ]

    def inner(a, b):
        terms = []
        for i in range(len(a)):
            for j in range(len(b)):
                terms.append((a[i] * b[j]) * gram[i][j])
        while len(terms) > 1:
            terms = [
                terms[i] + terms[i + 1] if i + 1 < len(terms) else terms[i]
                for i in range(0, len(terms), 2)
            ]
        return all_lanes(terms[0])

    centre = half + 1.0
    one = jnp.ones_like(half)
    none = jnp.zeros_like(half)
    res, direction, gain = [one], [one], [none] * ITERS
    current = inner(res, res)
    for iteration in range(ITERS):
        image = [centre * c for c in direction] + [none]
        for j, c in enumerate(direction):
            if j == 0:
                image[1] = image[1] + half * c
            else:
                image[j + 1] = image[j + 1] + 0.5 * half * c
                image[j - 1] = image[j - 1] + 0.5 * half * c
        step = current / inner(direction, image)
        for j, c in enumerate(direction):
            gain[j] = gain[j] + step * c
        res = [r - step * q for r, q in zip(res + [none], image)]
        if iteration < ITERS - 1:
            following = inner(res, res)
            ratio = following / current
            direction = [r + ratio * c for r, c in zip(res, direction + [none])]
            current = following

    lines = gain + res
    lines += [none] * (2 * SUB - len(lines))
    coef[...] = jnp.concatenate(lines, 0)


def finish_kernel(
    basis, state_ref, ds, vapour_ref, cos_ref, albedo_ref, net_ref, wide, wcol, maskv, coef,
    next_hbm, residual_hbm, net_hbm,
    next_ref, residual_ref, rest, scales, partial, sems,
):
    rows = vapour_ref.shape[0]
    done = edge(rows, WINDOWS)
    chunk = rows // 4
    early = pltpu.make_async_copy(
        net_ref.at[pl.ds(0, done)], net_hbm.at[pl.ds(0, done)], sems.at[0, 0]
    )
    early.start()
    lines = [coef[m:m + 1, :] for m in range(2 * ITERS + 1)]
    gain, res = lines[:ITERS], lines[ITERS:]
    copies = []
    for c in range(rows // chunk):
        @pl.loop(c * chunk, (c + 1) * chunk, unroll=chunk)
        def _(j):
            base = [basis[k, j + 1] for k in range(ITERS + 1)]
            scale = lax.rsqrt(ds[j + 1])
            moved, left = gain[0] * base[0], res[0] * base[0]
            for k in range(1, ITERS + 1):
                if k < ITERS:
                    moved = moved + gain[k] * base[k]
                left = left + res[k] * base[k]
            next_ref[j] = state_ref[j] + (scale * moved).T
            residual_ref[j] = (scale * left).T

        part = pl.ds(c * chunk, chunk)
        for i, (source, target) in enumerate([(next_ref, next_hbm), (residual_ref, residual_hbm)]):
            copies.append(pltpu.make_async_copy(source.at[part], target.at[part], sems.at[1 + i, c]))
            copies[-1].start()

    for j in range(done, rows):
        radiate(
            j, state_ref[j], vapour_ref, cos_ref, albedo_ref, maskv, wcol, wide, scales,
            partial, rest,
        )
    late = pltpu.make_async_copy(
        rest.at[pl.ds(done, rows - done)], net_hbm.at[pl.ds(done, rows - done)], sems.at[0, 1]
    )
    late.start()
    for copy in [early] + copies + [late]:
        copy.wait()


def body(mesh_shape, state_prev, diffusivity, vapour, cos_zenith, albedo, absorption, solar_weight, day_mask):
    nx, ny = mesh_shape
    rows, levels, lanes = state_prev.shape
    gpoints = absorption.shape[1]
    weight = solar_weight[None, :]
    absorb = absorption.T
    vmem = pl.BlockSpec(memory_space=pltpu.VMEM)
    hbm = pl.BlockSpec(memory_space=pltpu.HBM)
    dma = pltpu.SemaphoreType.DMA
    kinds = ITERS + 2
    cells = (rows, levels, lanes)
    turned = (rows, lanes, levels)
    around = (rows + 2, lanes, levels)
    scales = pltpu.VMEM((2, levels, lanes), F32)
    partial = pltpu.VMEM((levels * SUB, lanes), F32)
    held = pl.pallas_call(
        functools.partial(solve_kernel, nx, ny),
        out_shape=[
            pltpu.VMEM((ITERS + 1,) + around, F32),
            pltpu.VMEM(cells, F32),
            pltpu.VMEM(around, F32),
            pltpu.VMEM(cells, F32),
            pltpu.VMEM((rows, lanes), F32),
            pltpu.VMEM((rows, lanes), F32),
            pltpu.VMEM(cells, F32),
            pltpu.VMEM((levels, gpoints, lanes), F32),
            pltpu.VMEM((gpoints, lanes), F32),
            pltpu.VMEM((rows, lanes), F32),
            pltpu.VMEM((2 * SUB, levels), F32),
        ],
        in_specs=[hbm] * 8,
        out_specs=[vmem] * 11,
        scratch_shapes=[
            pltpu.VMEM(around, F32),
            pltpu.VMEM(cells, F32),
            pltpu.VMEM(around, F32),
            pltpu.VMEM(turned, F32),
            pltpu.VMEM(turned, F32),
            pltpu.VMEM(turned, F32),
            pltpu.VMEM((gpoints, levels), F32),
            pltpu.VMEM((1, gpoints), F32),
            pltpu.SMEM((rows,), jnp.int32),
            pltpu.VMEM((kinds, 2, rows, levels), F32),
            pltpu.VMEM((kinds, 2, rows, levels), F32),
            pltpu.VMEM((2, rows, levels), F32),
            scales,
            partial,
            pltpu.VMEM((2 * ITERS + 1, SUB, levels), F32),
            pltpu.VMEM((2, 2 * SUB, levels), F32),
            pltpu.VMEM((2, nx, 2 * SUB, levels), F32),
            pltpu.VMEM((2, 2 * SUB, levels), F32),
            pltpu.VMEM((2, ny, 2 * SUB, levels), F32),
            dma((8,)),
            dma((kinds, 2)), dma((kinds, 2)), dma((kinds, 2)), dma((kinds, 2)),
            dma((2, nx)), dma((2, nx)), dma((2, ny)), dma((2, ny)),
        ],
        compiler_params=pltpu.CompilerParams(
            collective_id=0, has_side_effects=True, vmem_limit_bytes=18 * 1024 * 1024
        ),
    )(*[
        pltpu.with_memory_space_constraint(a, pltpu.HBM)
        for a in (state_prev, diffusivity, vapour, cos_zenith, albedo, day_mask, absorb, weight)
    ])
    held = [pltpu.with_memory_space_constraint(h, pltpu.VMEM) for h in held]
    out = jax.ShapeDtypeStruct(cells, F32)
    return pl.pallas_call(
        finish_kernel,
        out_shape=(out, out, out),
        in_specs=[vmem] * 11,
        out_specs=(hbm, hbm, hbm),
        scratch_shapes=[
            pltpu.VMEM(cells, F32),
            pltpu.VMEM(cells, F32),
            pltpu.VMEM(cells, F32),
            scales,
            partial,
            dma((3, 4)),
        ],
        compiler_params=pltpu.CompilerParams(vmem_limit_bytes=8 * 1024 * 1024),
    )(*held)


def solution(mesh):
    cells = P("gy", None, "gx")
    columns = P("gy", "gx")
    return jax.shard_map(
        functools.partial(body, (mesh.shape["gx"], mesh.shape["gy"])),
        mesh=mesh,
        in_specs=(cells, cells, cells, columns, columns, P(), P(), P(("gx", "gy"))),
        out_specs=(cells, cells, cells),
        check_vma=False,
    )
```
